32 devices in a mesh: space: 4 (over y, x), sub: 8 (over z, core).
Axes of the slice: x: 2, y: 2, z: 4, core: 2. Of those that a mesh axis runs over, the one named last changes fastest.
Arguments:
- positions: float32 [3, 4, 512, 128], P(None, 'space', 'sub'), may hold values from 0 to 1.5
- masses: float32 [4, 512, 128], P('space', 'sub'), may hold values from 0.1 to 1
- occupancy: int32 [4, 512], P('space', 'sub'), may hold values from 1 to 128
- export_slots: int32 [4, 256], P('space', 'sub'), may hold values from 0 to 63, as said below
- export_count: int32 [4, 8], P('space', 'sub'), may hold values from 16 to 32
- pair_list: int32 [2, 4, 512], P(None, 'space', 'sub'), may hold values from 0 to 319, as said below
- pair_count: int32 [4, 8], P('space', 'sub'), may hold values from 16 to 64
Outputs:
- forces: float32 [3, 4, 512, 128], P(None, 'space', 'sub')
The draws below stay inside these ranges and needn't reach their ends.
Inputs may be any that keep to these rules, and one draw needn't show every extreme that they name: `export_slots`: the 32 entries of one device are distinct own-leaf indices. `pair_list`: row 0 is a target own leaf, below 64; row 1 is a source pool leaf, below 320, never equal to the target.
All inputs are finite; a program needn't handle non-finite values.
Results may differ from the reference program's by a relative error of at most 0.0003.
Values sent between devices are 32-bit elements; how exact they have to be, the bound alone decides.
A program may use at most 64 MiB of HBM per device.

```python
import math
import jax
import jax.numpy as jnp
from jax import lax

LEAF = 128
LEAVES = 64
G = 32
PAIRS = 64
N_SPACE = 4
N_SUB = 8


def draw_export_slots(key, part):
    keys = jax.random.split(jax.random.fold_in(key, 7), N_SPACE * N_SUB)
    chosen = jax.vmap(lambda single: jax.random.permutation(single, LEAVES)[:G])(keys)
    return chosen.reshape(N_SPACE, N_SUB * G).astype(jnp.int32)


def draw_pair_list(key, part):
    first, second = jax.random.split(jax.random.fold_in(key, 11))
    targets = jax.random.randint(first, (N_SPACE, N_SUB * PAIRS), 0, LEAVES, dtype=jnp.int32)
    drawn = jax.random.randint(second, (N_SPACE, N_SUB * PAIRS), 0, LEAVES + 8 * G - 1, dtype=jnp.int32)
    sources = drawn + (drawn >= targets).astype(jnp.int32)
    return jnp.stack([targets, sources]).astype(jnp.int32)


def plant(values, stream_key, smallest, largest):
    spot = [jax.random.randint(jax.random.fold_in(stream_key, axis), (), 0, length) for axis, length in enumerate(values.shape)]
    longest = values.shape.index(max(values.shape))
    neighbour = spot[:longest] + [(spot[longest] + 1) % values.shape[longest]] + spot[longest + 1:]
    return values.at[tuple(spot)].set(smallest).at[tuple(neighbour)].set(largest)


def block_levels(stream_key, extent, cuts, least, high):
    level, own = 1.0, jax.random.fold_in(stream_key, 6)
    for position, shards_of in cuts:
        draws = jnp.exp(jax.random.uniform(jax.random.fold_in(own, position), (shards_of,), jnp.float32, least / len(cuts), high / len(cuts)))
        level = level * jnp.repeat(draws, extent[position] // shards_of).reshape([-1 if axis == position else 1 for axis in range(len(extent))])
    return level


def setup_inputs(seed: int = 0) -> dict:
    splits = jax.random.split(jax.random.key(seed), 8)
    positions = jnp.clip(1.5 * jax.random.uniform(splits[0], (3, N_SPACE, N_SUB * LEAVES, LEAF), jnp.float32) ** block_levels(splits[0], (3, N_SPACE, N_SUB * LEAVES, LEAF), ((1, 4), (2, 8)), -0.2, 0.2), 0.0, 1.5)
    masses = jnp.clip(jnp.exp(math.log(1.0) - 2.3025851 * jax.random.uniform(splits[1], (N_SPACE, N_SUB * LEAVES, LEAF), jnp.float32) ** block_levels(splits[1], (N_SPACE, N_SUB * LEAVES, LEAF), ((0, 4), (1, 8)), -0.2, 0.2)), 0.1, 1.0)
    occupancy = plant(jax.random.randint(splits[2], (N_SPACE, N_SUB * LEAVES), 1, LEAF + 1), jax.random.fold_in(splits[2], 1), 1, LEAF).astype(jnp.int32)
    export_slots = draw_export_slots(jax.random.fold_in(splits[7], 71), 0)
    export_count = plant(jax.random.randint(splits[4], (N_SPACE, N_SUB), G // 2, G + 1), jax.random.fold_in(splits[4], 1), G // 2, G).astype(jnp.int32)
    pair_list = draw_pair_list(jax.random.fold_in(splits[7], 71), 0)
    pair_count = plant(jax.random.randint(splits[6], (N_SPACE, N_SUB), PAIRS // 4, PAIRS + 1), jax.random.fold_in(splits[6], 1), PAIRS // 4, PAIRS).astype(jnp.int32)
    return dict(positions=positions, masses=masses, occupancy=occupancy, export_slots=export_slots, export_count=export_count, pair_list=pair_list, pair_count=pair_count)


OFFSETS = ((-1, -1), (-1, 0), (-1, 1), (0, -1), (0, 1), (1, -1), (1, 0), (1, 1))
SOFTEN = 0.05
PRECISE = lax.Precision.HIGHEST

def pair_block(target_pos, target_mass, source_pos, source_mass):
    separation = source_pos[:, :, None, :] - target_pos[:, :, :, None]
    distance = lax.optimization_barrier(jnp.sum(separation * separation, axis=0))
    falloff = jnp.maximum(1.0 - distance, 0.0)
    softened = distance + SOFTEN
    weight = target_mass[:, :, None] * source_mass[:, None, :] * falloff * falloff / (softened * jnp.sqrt(softened))
    row_total = lax.optimization_barrier(jnp.sum(weight, axis=2))
    col_total = lax.optimization_barrier(jnp.sum(weight, axis=1))
    on_target = jnp.einsum('bij,cbj->cbi', weight, source_pos, precision=PRECISE) - target_pos * row_total[None]
    on_source = jnp.einsum('bij,cbi->cbj', weight, target_pos, precision=PRECISE) - source_pos * col_total[None]
    return (on_target, on_source)

def device_forces(pool_pos, pool_mass, pair_rows, pair_total):
    own_index = jnp.arange(LEAVES, dtype=jnp.int32)
    live = (jnp.arange(PAIRS, dtype=jnp.int32) < pair_total).astype(jnp.float32)
    targets = jnp.concatenate([own_index, pair_rows[0]])
    sources = jnp.concatenate([own_index, pair_rows[1]])
    target_scale = jnp.concatenate([jnp.ones((LEAVES,), jnp.float32), live])
    source_scale = jnp.concatenate([jnp.zeros((LEAVES,), jnp.float32), live])

    def one_block(indices):
        tgt_rows, src_rows = indices
        return pair_block(pool_pos[:, tgt_rows], pool_mass[tgt_rows], pool_pos[:, src_rows], pool_mass[src_rows])
    on_target, on_source = lax.map(one_block, (targets.reshape(8, -1), sources.reshape(8, -1)))
    on_target = jnp.moveaxis(on_target, 0, 1).reshape(3, -1, LEAF)
    on_source = jnp.moveaxis(on_source, 0, 1).reshape(3, -1, LEAF)
    pool_force = jnp.zeros((3, pool_mass.shape[0], LEAF), jnp.float32)
    pool_force = pool_force.at[:, targets].add(on_target * target_scale[None, :, None])
    pool_force = pool_force.at[:, sources].add(on_source * source_scale[None, :, None])
    return pool_force

def reference(positions, masses, occupancy, export_slots, export_count, pair_list, pair_count):
    slot_index = lax.broadcasted_iota(jnp.int32, masses.shape, 2)
    live_mass = jnp.where(slot_index < occupancy[:, :, None], masses, 0.0)
    grid_pos = positions.reshape(3, N_SPACE, N_SUB, LEAVES, LEAF)
    grid_mass = live_mass.reshape(N_SPACE, N_SUB, LEAVES, LEAF)
    slots = export_slots.reshape(N_SPACE, N_SUB, G)
    keep = (jnp.arange(G, dtype=jnp.int32)[None, None, :] < export_count[:, :, None]).astype(jnp.float32)
    pos_index = jnp.broadcast_to(slots[None, :, :, :, None], (3, N_SPACE, N_SUB, G, LEAF))
    mass_index = jnp.broadcast_to(slots[:, :, :, None], (N_SPACE, N_SUB, G, LEAF))
    sent_pos = jnp.take_along_axis(grid_pos, pos_index, axis=3)
    sent_mass = jnp.take_along_axis(grid_mass, mass_index, axis=2) * keep[:, :, :, None]
    pos_list = [grid_pos]
    mass_list = [grid_mass]
    for space_step, sub_step in OFFSETS:
        pos_list.append(jnp.roll(sent_pos, (-space_step, -sub_step), axis=(1, 2)))
        mass_list.append(jnp.roll(sent_mass, (-space_step, -sub_step), axis=(0, 1)))
    pool_pos = jnp.concatenate(pos_list, axis=3)
    pool_mass = jnp.concatenate(mass_list, axis=2)
    pool_size = LEAVES + 8 * G
    device_total = N_SPACE * N_SUB
    dev_pos = jnp.moveaxis(pool_pos.reshape(3, device_total, pool_size, LEAF), 1, 0)
    dev_mass = pool_mass.reshape(device_total, pool_size, LEAF)
    dev_pairs = jnp.moveaxis(pair_list.reshape(2, device_total, PAIRS), 1, 0)
    dev_count = pair_count.reshape(device_total)

    def per_device(items):
        return device_forces(items[0], items[1], items[2], items[3])
    pool_force = lax.map(per_device, (dev_pos, dev_mass, dev_pairs, dev_count))
    pool_force = pool_force.reshape(N_SPACE, N_SUB, 3, pool_size, LEAF)
    own_force = pool_force[:, :, :, :LEAVES]
    returned = jnp.zeros((N_SPACE, N_SUB, 3, G, LEAF), jnp.float32)
    for order, (space_step, sub_step) in enumerate(OFFSETS):
        block = pool_force[:, :, :, LEAVES + order * G:LEAVES + (order + 1) * G]
        returned = returned + jnp.roll(block, (space_step, sub_step), axis=(0, 1))
    picker = (slots[:, :, :, None] == jnp.arange(LEAVES, dtype=jnp.int32)[None, None, None, :]).astype(jnp.float32)
    own_force = own_force + jnp.einsum('sbgl,sbcgp->sbclp', picker, returned, precision=PRECISE)
    forces = jnp.moveaxis(own_force, 2, 0)
    return forces.reshape(3, N_SPACE, N_SUB * LEAVES, LEAF)
```

```python
import functools

import jax
import jax.numpy as jnp
from jax import lax
from jax.experimental import pallas as pl
from jax.experimental.pallas import tpu as pltpu
from jax.sharding import PartitionSpec as P

OFFSETS = ((-1, -1), (-1, 0), (-1, 1), (0, -1), (0, 1), (1, -1), (1, 0), (1, 1))
SOFTEN = 0.05
CENTRE = 0.75
MESH = pl.DeviceIdType.MESH
F32, BF16 = jnp.float32, jnp.bfloat16
UNROLL = 16
CHUNKS = 1
CUTS = (12, 16)
PAIR_CUTS = (4, 8, 12, 16)


def split3(v):
    high = v.astype(BF16).astype(F32)
    rest = v - high
    mid = rest.astype(BF16).astype(F32)
    return high, mid, rest - mid


def rows_of(sub, values):
    out = jnp.zeros(sub.shape, F32)
    for index, value in enumerate(values):
        out = jnp.where(sub == index, value, out)
    return out


def kernel(pos_in, mass_in, occ_in, slots_in, count_in, pairs_in, live_in, out,
           pos, mass, occ, occ_s, slots_v, slots_s, count_s, pairs_v, pairs_s, live_s,
           pool, export, turned, kept, self_res, tgt_res, src_res, ghost, came, crossing,
           load_sem, send_sem, recv_sem, back_recv):
    leaves, width = mass.shape[1:]
    sent = slots_s.shape[1]
    pairs = pairs_s.shape[2]
    block_rows = 4 * sent
    own_blocks = leaves // sent
    n_space, n_sub = lax.axis_size("space"), lax.axis_size("sub")
    s, r = lax.axis_index("space"), lax.axis_index("sub")
    device = {
        (-1, 0): (lax.rem(s + n_space - 1, n_space), r),
        (1, 0): (lax.rem(s + 1, n_space), r),
        (0, -1): (s, lax.rem(r + n_sub - 1, n_sub)),
        (0, 1): (s, lax.rem(r + 1, n_sub)),
    }
    barrier = pltpu.get_barrier_semaphore()
    for where in device.values():
        pl.semaphore_signal(barrier, inc=1, device_id=where, device_id_type=MESH)
    loads = [
        pltpu.make_async_copy(source, target, load_sem.at[index])
        for index, (source, target) in enumerate((
            (slots_in, slots_s), (occ_in, occ_s), (count_in, count_s), (pos_in, pos),
            (mass_in, mass), (occ_in, occ), (slots_in, slots_v), (pairs_in, pairs_v),
            (pairs_in, pairs_s), (live_in, live_s),
        ))
    ]
    for copy in loads:
        copy.start()
    for copy in loads[:5]:
        copy.wait()

    def row(leaf, c):
        return lax.div(leaf, sent) * block_rows + lax.rem(leaf, sent) + c * sent

    def load(leaf):
        start = row(leaf, 0)
        return [pool[pl.ds(start + c * sent, 1), :] for c in range(4)]

    lane_row = lax.broadcasted_iota(jnp.int32, (1, width), 1)
    for g in range(sent):
        slot = slots_s[0, g]
        filled = jnp.where(g < count_s[0, 0], occ_s[0, slot], 0)
        for c in range(3):
            export[pl.ds(c * sent + g, 1), :] = pos[c, 0, pl.ds(slot, 1), :] - CENTRE
        export[pl.ds(3 * sent + g, 1), :] = jnp.where(
            lane_row < filled, mass[0, pl.ds(slot, 1), :], 0.0
        )

    sub = lax.broadcasted_iota(jnp.int32, (8, width), 0)
    low = sub < 4

    chunk_rows = block_rows // CHUNKS
    direct = ((-1, 0), (1, 0), (0, -1), (0, 1))

    def send(source, towards, arrives, chunk):
        index = OFFSETS.index(arrives)
        start = (own_blocks + index) * block_rows + chunk * chunk_rows
        return pltpu.make_async_remote_copy(
            src_ref=source, dst_ref=pool.at[pl.ds(start, chunk_rows), :],
            send_sem=send_sem.at[0], recv_sem=recv_sem.at[2 if arrives[1] else (arrives[0] + 1) // 2, chunk],
            device_id=device[towards], device_id_type=MESH,
        )

    def whole(ref, sem):
        return pltpu.make_async_remote_copy(
            src_ref=ref, dst_ref=ref, send_sem=sem, recv_sem=sem,
            device_id=device[(0, 1)], device_id_type=MESH,
        )

    copies = {}
    for chunk in range(CHUNKS):
        for a, b in direct:
            source = export.at[pl.ds(chunk * chunk_rows, chunk_rows), :]
            copies[(a, b, chunk)] = send(source, (-a, -b), (a, b), chunk)
        for a in (-1, 1):
            start = (own_blocks + OFFSETS.index((a, 0))) * block_rows + chunk * chunk_rows
            for b in (-1, 1):
                source = pool.at[pl.ds(start, chunk_rows), :]
                copies[(a, b, chunk)] = send(source, (0, -b), (a, b), chunk)

    pl.semaphore_wait(barrier, 4)
    for near in (direct[:2], direct[2:]):
        for chunk in range(CHUNKS):
            for a, b in near:
                copies[(a, b, chunk)].start()

    for copy in loads[5:]:
        copy.wait()
    eye = (
        lax.broadcasted_iota(jnp.int32, (leaves, leaves), 0)
        == lax.broadcasted_iota(jnp.int32, (leaves, leaves), 1)
    )
    occ_col = jnp.sum(jnp.where(eye, occ[...].astype(F32), 0.0), axis=1, keepdims=True)
    lane = lax.broadcasted_iota(jnp.int32, (leaves, width), 1).astype(F32)
    own_mass = jnp.where(lane < occ_col, mass[0], 0.0)
    for block in range(own_blocks):
        part = slice(block * sent, (block + 1) * sent)
        for c in range(3):
            pool[pl.ds(block * block_rows + c * sent, sent), :] = pos[c, 0, part] - CENTRE
        pool[pl.ds(block * block_rows + 3 * sent, sent), :] = own_mass[part]

    def features(x, y, z):
        q = x * x + y * y + z * z
        return rows_of(sub, (x, y, z, 1.0, q + SOFTEN)), q

    def right_operand(vb):
        h, m, l = split3(vb)
        return jnp.concatenate([h, m, h, l, h, m], axis=0).astype(BF16)

    def left_operand(vb, q):
        va = jnp.where(sub < 3, -2.0 * vb, rows_of(sub, (0.0, 0.0, 0.0, q, 1.0)))
        h, m, l = split3(va)
        return jnp.concatenate([h, h, m, h, l, m], axis=0)

    def force_operand(vb, m):
        moment = m * rows_of(sub, (vb[0:1], vb[1:2], vb[2:3], 1.0, vb[0:1], vb[1:2], vb[2:3], 1.0))
        h, mid, l = split3(moment)
        both = jnp.concatenate([jnp.where(low, h, mid), jnp.where(low, l, 0.0)], axis=0).astype(BF16)
        return jnp.concatenate([both, both], axis=1)

    def weights(left, right):
        soft = jnp.dot(left, right, preferred_element_type=F32)
        fall = jnp.maximum((1.0 + SOFTEN) - soft, 0.0)
        root = lax.rsqrt(soft)
        part = fall * root
        weight = part * part * root
        high = weight.astype(BF16)
        rest = (weight - high.astype(F32)).astype(BF16)
        return high, rest

    def finish(product, vb, m):
        total = product[:8] + pltpu.roll(product[:8], 4, 0) + product[8:]
        return m * (total - vb * total[3:4])

    def self_pair(leaf):
        x, y, z, m = load(leaf)
        vb, q = features(x, y, z)
        left = jnp.transpose(left_operand(vb, q)).astype(BF16)
        turned[leaf] = left
        high, rest = weights(left, right_operand(vb))
        product = jnp.dot(
            force_operand(vb, m), jnp.concatenate([high, rest], axis=0), preferred_element_type=F32
        )
        self_res[pl.ds(pl.multiple_of(leaf * 8, 8), 8), :] = finish(product, vb, m)

    def listed_pair(p):
        target, source = pairs_s[0, 0, p], pairs_s[1, 0, p]
        x, y, z, m_t = load(target)
        vb_t, _ = features(x, y, z)
        x, y, z, m_u = load(source)
        vb_u, _ = features(x, y, z)
        high, rest = weights(turned[target], right_operand(vb_u))
        onto_source = jnp.dot(
            force_operand(vb_t, m_t), jnp.concatenate([high, rest], axis=0),
            preferred_element_type=F32,
        )
        kept[p, :, :width] = high
        kept[p, :, width:] = rest
        src_res[pl.ds(pl.multiple_of(p * 8, 8), 8), :] = finish(onto_source, vb_u, m_u)

    def target_side(p):
        target, source = pairs_s[0, 0, p], pairs_s[1, 0, p]
        x, y, z, m_t = load(target)
        vb_t, _ = features(x, y, z)
        x, y, z, m_u = load(source)
        vb_u, _ = features(x, y, z)
        onto_target = lax.dot_general(
            force_operand(vb_u, m_u), kept[p], (((1,), (1,)), ((), ())),
            preferred_element_type=F32,
        )
        tgt_res[pl.ds(pl.multiple_of(p * 8, 8), 8), :] = finish(onto_target, vb_t, m_t)

    def run(body, first, last):
        def step(i, carry):
            for j in range(UNROLL):
                body(first + i * UNROLL + j)
            return carry

        lax.fori_loop(0, (last - first) // UNROLL, step, 0)

    cuts = [leaves * cut // 16 for cut in CUTS]
    run(self_pair, 0, cuts[0])
    for chunk in range(CHUNKS):
        for a in (-1, 1):
            copies[(a, 0, chunk)].wait_recv()
            for b in (-1, 1):
                copies[(a, b, chunk)].start()
        run(self_pair, cuts[chunk], cuts[chunk + 1])
    for chunk in range(CHUNKS):
        sub_rows = pl.ds(own_blocks * block_rows, 6 * chunk_rows)
        whole(pool.at[sub_rows, :], recv_sem.at[2, chunk]).wait_recv()
    run(listed_pair, 0, pairs)

    def component(ref, c, count):
        return ref[pl.ds(c, count, stride=8), :]

    def stacked(values):
        return jnp.concatenate([part for part in split3(values)], axis=0).astype(BF16)

    pair_live = lax.broadcasted_iota(jnp.int32, (1, pairs), 1) < live_s[0, 0]

    def onehot(rows, start, wanted, live):
        which = lax.broadcasted_iota(jnp.int32, (rows, wanted.shape[1]), 0) + start
        hit = which == wanted
        if live is not None:
            hit = jnp.logical_and(hit, live)
        hit = jnp.where(hit, 1.0, 0.0)
        return hit

    tgt_row, src_row = pairs_v[0], pairs_v[1]
    src_parts = [stacked(component(src_res, c, pairs)) for c in range(3)]
    src_all = jnp.concatenate(src_parts, axis=1)
    hit = onehot(8 * sent, leaves, src_row, pair_live)
    onto_ghost = jnp.concatenate([hit, hit, hit], axis=1).astype(BF16)
    ghost_force = jnp.dot(onto_ghost, src_all, preferred_element_type=F32)
    for k in range(8):
        for c in range(3):
            ghost[k, pl.ds(c * sent, sent), :] = ghost_force[
                k * sent:(k + 1) * sent, c * width:(c + 1) * width
            ]

    def give(source, slot, towards, c):
        return pltpu.make_async_remote_copy(
            src_ref=source, dst_ref=came.at[c, slot],
            send_sem=send_sem.at[1], recv_sem=back_recv.at[slot // 4, c],
            device_id=device[towards], device_id_type=MESH,
        )

    def part(c):
        return pl.ds(c * sent, sent)

    back = {}
    for near in ((-1, 1), (0,)):
        for c in range(3):
            for a in near:
                for b in (-1, 1):
                    slot = {-1: 0, 1: 2, 0: 4}[a] + (b + 1) // 2
                    back[(a, b, c)] = give(
                        ghost.at[OFFSETS.index((a, b)), part(c), :], slot, (0, b), c
                    )
                    back[(a, b, c)].start()

    def arrived(a, c):
        first = {-1: 0, 1: 2, 0: 4}[a]
        return came[c, first] + came[c, first + 1]

    pair_cuts = [pairs * cut // 16 for cut in PAIR_CUTS]
    run(target_side, 0, pair_cuts[0])
    for c in range(3):
        whole(came.at[c, pl.ds(0, 4)], back_recv.at[0, c]).wait_recv()
        for a in (-1, 1):
            side = (a + 1) // 2
            crossing[side, part(c), :] = ghost[OFFSETS.index((a, 0)), part(c), :] + arrived(a, c)
            back[(a, 0, c)] = give(
                crossing.at[side, part(c), :], 6 + side, (a, 0), c
            )
            back[(a, 0, c)].start()
        run(target_side, pair_cuts[c], pair_cuts[c + 1])
    tgt_all = jnp.concatenate([stacked(component(tgt_res, c, pairs)) for c in range(3)], axis=1)
    hit_t = onehot(leaves, 0, tgt_row, pair_live)
    hit_s = onehot(leaves, 0, src_row, pair_live)
    own_force = jnp.dot(
        jnp.concatenate([hit_t, hit_t, hit_t, hit_s, hit_s, hit_s], axis=1).astype(BF16),
        jnp.concatenate([tgt_all, src_all], axis=0), preferred_element_type=F32,
    )

    returned = []
    for c in range(3):
        whole(came.at[c, pl.ds(4, 4)], back_recv.at[1, c]).wait_recv()
        returned.append(stacked(arrived(0, c) + came[c, 6] + came[c, 7]))
    parts = jnp.concatenate(returned, axis=1)
    hit = onehot(leaves, 0, slots_v[...], None)
    own_force = own_force + jnp.dot(
        jnp.concatenate([hit, hit, hit], axis=1).astype(BF16), parts, preferred_element_type=F32
    )
    for c in range(3):
        out[c, 0] = component(self_res, c, leaves) + own_force[:, c * width:(c + 1) * width]
    whole(pool.at[pl.ds(own_blocks * block_rows, 8 * block_rows), :], send_sem.at[0]).wait_send()
    whole(ghost, send_sem.at[1]).wait_send()


def local(positions, masses, occupancy, export_slots, export_count, pair_list, pair_count):
    leaves, width = masses.shape[1:]
    sent = export_slots.shape[1]
    pairs = pair_list.shape[2]
    return pl.pallas_call(
        kernel,
        out_shape=pltpu.VMEM(positions.shape, F32),
        in_specs=[pl.BlockSpec(memory_space=pl.ANY)] * 7,
        out_specs=pl.BlockSpec(memory_space=pltpu.VMEM),
        scratch_shapes=[
            pltpu.VMEM(positions.shape, F32),
            pltpu.VMEM(masses.shape, F32),
            pltpu.VMEM(occupancy.shape, jnp.int32),
            pltpu.SMEM(occupancy.shape, jnp.int32),
            pltpu.VMEM(export_slots.shape, jnp.int32),
            pltpu.SMEM(export_slots.shape, jnp.int32),
            pltpu.SMEM(export_count.shape, jnp.int32),
            pltpu.VMEM(pair_list.shape, jnp.int32),
            pltpu.SMEM(pair_list.shape, jnp.int32),
            pltpu.SMEM(pair_count.shape, jnp.int32),
            pltpu.VMEM((4 * (leaves + 8 * sent), width), F32),
            pltpu.VMEM((4 * sent, width), F32),
            pltpu.VMEM((leaves, width, 48), BF16),
            pltpu.VMEM((pairs, width, 2 * width), BF16),
            pltpu.VMEM((8 * leaves, width), F32),
            pltpu.VMEM((8 * pairs, width), F32),
            pltpu.VMEM((8 * pairs, width), F32),
            pltpu.VMEM((8, 3 * sent, width), F32),
            pltpu.VMEM((3, 8, sent, width), F32),
            pltpu.VMEM((2, 3 * sent, width), F32),
            pltpu.SemaphoreType.DMA((10,)),
            pltpu.SemaphoreType.DMA((2,)),
            pltpu.SemaphoreType.DMA((3, CHUNKS)),
            pltpu.SemaphoreType.DMA((2, 3)),
        ],
        compiler_params=pltpu.CompilerParams(collective_id=0, has_side_effects=True),
    )(positions, masses, occupancy, export_slots, export_count, pair_list, pair_count)


def solution(mesh):
    return jax.shard_map(
        local,
        mesh=mesh,
        in_specs=(
            P(None, "space", "sub", None),
            P("space", "sub", None),
            P("space", "sub"),
            P("space", "sub"),
            P("space", "sub"),
            P(None, "space", "sub"),
            P("space", "sub"),
        ),
        out_specs=P(None, "space", "sub", None),
        check_vma=False,
    )
```

```python
import functools

import jax
import jax.numpy as jnp
from jax import lax
from jax.experimental import pallas as pl
from jax.experimental.pallas import tpu as pltpu
from jax.sharding import PartitionSpec as P

OFFSETS = ((-1, -1), (-1, 0), (-1, 1), (0, -1), (0, 1), (1, -1), (1, 0), (1, 1))
SOFTEN = 0.05
CENTRE = 0.75
MESH = pl.DeviceIdType.MESH
F32, BF16 = jnp.float32, jnp.bfloat16
UNROLL = 16
CHUNKS = 2
CUTS = (12, 16, 16)


def split3(v):
    high = v.astype(BF16).astype(F32)
    rest = v - high
    mid = rest.astype(BF16).astype(F32)
    return high, mid, rest - mid


def rows_of(sub, values):
    out = jnp.zeros(sub.shape, F32)
    for index, value in enumerate(values):
        out = jnp.where(sub == index, value, out)
    return out


def kernel(pos_in, mass_in, occ_in, slots_in, count_in, pairs_in, live_in, out,
           pos, mass, occ, occ_s, slots_v, slots_s, count_s, pairs_v, pairs_s, live_s,
           pool, export, turned, kept, self_res, tgt_res, src_res, ghost, came, crossing,
           load_sem, send_sem, recv_sem, back_recv):
    leaves, width = mass.shape[1:]
    sent = slots_s.shape[1]
    pairs = pairs_s.shape[2]
    block_rows = 4 * sent
    own_blocks = leaves // sent
    n_space, n_sub = lax.axis_size("space"), lax.axis_size("sub")
    s, r = lax.axis_index("space"), lax.axis_index("sub")
    device = {
        (a, b): (lax.rem(s + n_space + a, n_space), lax.rem(r + n_sub + b, n_sub))
        for a, b in OFFSETS
    }
    wraps = {-1: r == 0, 1: r == n_sub - 1}
    edge = jnp.logical_or(wraps[-1], wraps[1])
    barrier = pltpu.get_barrier_semaphore()

    def greet(where):
        pl.semaphore_signal(barrier, inc=1, device_id=where, device_id_type=MESH)

    @pl.when(wraps[-1])
    def _():
        for a in (-1, 1):
            greet(device[(a, -1)])

    for where in ((0, -1), (0, 1), (-1, 0), (1, 0)):
        greet(device[where])
    loads = [
        pltpu.make_async_copy(source, target, load_sem.at[index])
        for index, (source, target) in enumerate((
            (slots_in, slots_s), (occ_in, occ_s), (count_in, count_s), (pos_in, pos),
            (mass_in, mass), (occ_in, occ), (slots_in, slots_v), (pairs_in, pairs_v),
            (pairs_in, pairs_s), (live_in, live_s),
        ))
    ]
    for copy in loads:
        copy.start()
    for copy in loads[:5]:
        copy.wait()

    def row(leaf, c):
        return lax.div(leaf, sent) * block_rows + lax.rem(leaf, sent) + c * sent

    def load(leaf):
        start = row(leaf, 0)
        return [pool[pl.ds(start + c * sent, 1), :] for c in range(4)]

    lane_row = lax.broadcasted_iota(jnp.int32, (1, width), 1)
    for g in range(sent):
        slot = slots_s[0, g]
        filled = jnp.where(g < count_s[0, 0], occ_s[0, slot], 0)
        for c in range(3):
            export[pl.ds(c * sent + g, 1), :] = pos[c, 0, pl.ds(slot, 1), :] - CENTRE
        export[pl.ds(3 * sent + g, 1), :] = jnp.where(
            lane_row < filled, mass[0, pl.ds(slot, 1), :], 0.0
        )

    sub = lax.broadcasted_iota(jnp.int32, (8, width), 0)
    low = sub < 4

    chunk_rows = block_rows // CHUNKS

    def rows_at(index, chunk=None):
        start = (own_blocks + OFFSETS.index(index)) * block_rows
        if chunk is None:
            return pl.ds(start, block_rows)
        return pl.ds(start + chunk * chunk_rows, chunk_rows)

    def send(source, where, target, sem, sent_sem=0):
        return pltpu.make_async_remote_copy(
            src_ref=source, dst_ref=pool.at[target, :], send_sem=send_sem.at[sent_sem],
            recv_sem=recv_sem.at[sem], device_id=device[where], device_id_type=MESH,
        )

    def whole(ref, sem):
        return pltpu.make_async_remote_copy(
            src_ref=ref, dst_ref=ref, send_sem=sem, recv_sem=sem,
            device_id=device[(0, 1)], device_id_type=MESH,
        )

    rest = 2 * CHUNKS
    across = {
        (a, chunk): send(
            export.at[pl.ds(chunk * chunk_rows, chunk_rows), :], (-a, 0),
            rows_at((a, 0), chunk), 2 * chunk + (a + 1) // 2,
        )
        for chunk in range(CHUNKS) for a in (-1, 1)
    }

    def forward(a, b, chunk):
        rows = rows_at((a, 0), chunk)
        return send(pool.at[rows, :], (0, -b), rows_at((a, b), chunk), rest)

    pl.semaphore_wait(barrier, jnp.where(wraps[1], 6, 4))
    @pl.when(wraps[1])
    def _():
        for a in (-1, 1):
            send(export, (-a, 1), rows_at((a, -1)), rest).start()

    for copy in across.values():
        copy.start()
    for b in (-1, 1):
        send(export, (0, -b), rows_at((0, b)), rest + (b + 1) // 2).start()
    for copy in loads[5:]:
        copy.wait()
    eye = (
        lax.broadcasted_iota(jnp.int32, (leaves, leaves), 0)
        == lax.broadcasted_iota(jnp.int32, (leaves, leaves), 1)
    )
    occ_col = jnp.sum(jnp.where(eye, occ[...].astype(F32), 0.0), axis=1, keepdims=True)
    lane = lax.broadcasted_iota(jnp.int32, (leaves, width), 1).astype(F32)
    own_mass = jnp.where(lane < occ_col, mass[0], 0.0)
    for block in range(own_blocks):
        part = slice(block * sent, (block + 1) * sent)
        for c in range(3):
            pool[pl.ds(block * block_rows + c * sent, sent), :] = pos[c, 0, part] - CENTRE
        pool[pl.ds(block * block_rows + 3 * sent, sent), :] = own_mass[part]

    def features(x, y, z):
        q = x * x + y * y + z * z
        return rows_of(sub, (x, y, z, 1.0, q + SOFTEN)), q

    def right_operand(vb):
        h, m, l = split3(vb)
        return jnp.concatenate([h, m, h, l, h, m], axis=0).astype(BF16)

    def left_operand(vb, q):
        va = jnp.where(sub < 3, -2.0 * vb, rows_of(sub, (0.0, 0.0, 0.0, q, 1.0)))
        h, m, l = split3(va)
        return jnp.concatenate([h, h, m, h, l, m], axis=0)

    def force_operand(vb, m):
        moment = m * rows_of(sub, (vb[0:1], vb[1:2], vb[2:3], 1.0, vb[0:1], vb[1:2], vb[2:3], 1.0))
        h, mid, l = split3(moment)
        both = jnp.concatenate([jnp.where(low, h, mid), jnp.where(low, l, 0.0)], axis=0).astype(BF16)
        return jnp.concatenate([both, both], axis=1)

    def weights(left, right):
        soft = jnp.dot(left, right, preferred_element_type=F32)
        fall = jnp.maximum((1.0 + SOFTEN) - soft, 0.0)
        root = lax.rsqrt(soft)
        part = fall * root
        weight = part * part * root
        high = weight.astype(BF16)
        rest = (weight - high.astype(F32)).astype(BF16)
        return high, rest

    def finish(product, vb, m):
        total = product[:8] + pltpu.roll(product[:8], 4, 0) + product[8:]
        return m * (total - vb * total[3:4])

    def self_pair(leaf):
        x, y, z, m = load(leaf)
        vb, q = features(x, y, z)
        left = jnp.transpose(left_operand(vb, q)).astype(BF16)
        turned[leaf] = left
        high, rest = weights(left, right_operand(vb))
        product = jnp.dot(
            force_operand(vb, m), jnp.concatenate([high, rest], axis=0), preferred_element_type=F32
        )
        self_res[pl.ds(pl.multiple_of(leaf * 8, 8), 8), :] = finish(product, vb, m)

    def listed_pair(p):
        target, source = pairs_s[0, 0, p], pairs_s[1, 0, p]
        x, y, z, m_t = load(target)
        vb_t, _ = features(x, y, z)
        x, y, z, m_u = load(source)
        vb_u, _ = features(x, y, z)
        high, rest = weights(turned[target], right_operand(vb_u))
        onto_source = jnp.dot(
            force_operand(vb_t, m_t), jnp.concatenate([high, rest], axis=0),
            preferred_element_type=F32,
        )
        kept[p, :, :width] = high
        kept[p, :, width:] = rest
        src_res[pl.ds(pl.multiple_of(p * 8, 8), 8), :] = finish(onto_source, vb_u, m_u)

    def target_side(p):
        target, source = pairs_s[0, 0, p], pairs_s[1, 0, p]
        x, y, z, m_t = load(target)
        vb_t, _ = features(x, y, z)
        x, y, z, m_u = load(source)
        vb_u, _ = features(x, y, z)
        onto_target = lax.dot_general(
            force_operand(vb_u, m_u), kept[p], (((1,), (1,)), ((), ())),
            preferred_element_type=F32,
        )
        tgt_res[pl.ds(pl.multiple_of(p * 8, 8), 8), :] = finish(onto_target, vb_t, m_t)

    def run(body, first, last, unroll=UNROLL):
        def step(i, carry):
            for j in range(unroll):
                body(first + i * unroll + j)
            return carry

        lax.fori_loop(0, (last - first) // unroll, step, 0)

    cuts = [leaves * cut // 16 for cut in CUTS]
    run(self_pair, 0, cuts[0])
    for chunk in range(CHUNKS):
        for a in (-1, 1):
            across[(a, chunk)].wait_recv()
            for b in (-1, 1):
                @pl.when(jnp.logical_not(wraps[-b]))
                def _():
                    forward(a, b, chunk).start()
        run(self_pair, cuts[chunk], cuts[chunk + 1])
    ghosts = own_blocks * block_rows
    whole(pool.at[rows_at((0, 1)), :], recv_sem.at[rest + 1]).wait_recv()

    @pl.when(wraps[1])
    def _():
        for a in (-1, 1):
            send(pool.at[rows_at((0, 1)), :], (-a, 0), rows_at((a, 1)), rest, 2).start()

    whole(pool.at[pl.ds(ghosts, 5 * block_rows), :], recv_sem.at[rest]).wait_recv()
    run(listed_pair, 0, pairs, 64)

    def component(ref, c, count):
        return ref[pl.ds(c, count, stride=8), :]

    def stacked(values):
        return jnp.concatenate([part for part in split3(values)], axis=0).astype(BF16)

    pair_live = lax.broadcasted_iota(jnp.int32, (1, pairs), 1) < live_s[0, 0]

    def onehot(rows, start, wanted, live):
        which = lax.broadcasted_iota(jnp.int32, (rows, wanted.shape[1]), 0) + start
        hit = which == wanted
        if live is not None:
            hit = jnp.logical_and(hit, live)
        hit = jnp.where(hit, 1.0, 0.0)
        return hit

    tgt_row, src_row = pairs_v[0], pairs_v[1]
    src_parts = [stacked(component(src_res, c, pairs)) for c in range(3)]
    src_all = jnp.concatenate(src_parts, axis=1)
    hit = onehot(8 * sent, leaves, src_row, pair_live)
    onto_ghost = jnp.concatenate([hit, hit, hit], axis=1).astype(BF16)

    def part(c):
        return pl.ds(c * sent, sent)

    def slot_of(a, b):
        return {-1: 0, 1: 2, 0: 4}[a] + (b + 1) // 2

    def give(source, slot, where, c, last):
        return pltpu.make_async_remote_copy(
            src_ref=source, dst_ref=came.at[c, slot],
            send_sem=send_sem.at[1], recv_sem=back_recv.at[last, c],
            device_id=where, device_id_type=MESH,
        )

    for c in range(3):
        ghost_force = jnp.dot(onto_ghost, src_parts[c], preferred_element_type=F32)
        for k in range(8):
            ghost[k, part(c), :] = ghost_force[k * sent:(k + 1) * sent]
        for a in (-1, 1):
            for b in (-1, 1):
                to_space, to_sub = device[(a, b)]
                give(
                    ghost.at[OFFSETS.index((a, b)), part(c), :], slot_of(a, b),
                    (jnp.where(wraps[b], to_space, s), to_sub), c, jnp.where(wraps[b], 1, 0),
                ).start()
    for c in range(3):
        for b in (-1, 1):
            give(
                ghost.at[OFFSETS.index((0, b)), part(c), :], slot_of(0, b), device[(0, b)], c, 1
            ).start()

    def took(c, last, at_edge, inside):
        for which, count in ((edge, at_edge), (jnp.logical_not(edge), inside)):
            @pl.when(which)
            def _():
                whole(came.at[c, pl.ds(0, count)], back_recv.at[last, c]).wait_recv()

    for c in range(3):
        took(c, 0, 2, 4)

        for a in (-1, 1):
            side = (a + 1) // 2
            first = came[c, jnp.where(wraps[1], slot_of(a, 1), slot_of(a, -1))]
            second = came[c, jnp.where(wraps[-1], slot_of(a, -1), slot_of(a, 1))]
            crossing[side, part(c), :] = (
                ghost[OFFSETS.index((a, 0)), part(c), :] + first + jnp.where(edge, 0.0, second)
            )
            give(crossing.at[side, part(c), :], 6 + side, device[(a, 0)], c, 1).start()
    run(target_side, 0, pairs)
    tgt_all = jnp.concatenate([stacked(component(tgt_res, c, pairs)) for c in range(3)], axis=1)
    hit_t = onehot(leaves, 0, tgt_row, pair_live)
    hit_s = onehot(leaves, 0, src_row, pair_live)
    own_force = jnp.dot(
        jnp.concatenate([hit_t, hit_t, hit_t, hit_s, hit_s, hit_s], axis=1).astype(BF16),
        jnp.concatenate([tgt_all, src_all], axis=0), preferred_element_type=F32,
    )

    hit = onehot(leaves, 0, slots_v[...], None)
    onto_own = jnp.concatenate([hit, hit, hit], axis=1).astype(BF16)
    own_force = [
        component(self_res, c, leaves) + own_force[:, c * width:(c + 1) * width] for c in range(3)
    ]
    for c in range(3):
        took(c, 1, 6, 4)

        far = [came[c, jnp.where(wraps[-1], slot_of(a, 1), slot_of(a, -1))] for a in (-1, 1)]
        returned = stacked(
            came[c, 4] + came[c, 5] + came[c, 6] + came[c, 7] + jnp.where(edge, far[0] + far[1], 0.0)
        )
        out[c, 0] = own_force[c] + jnp.dot(onto_own, returned, preferred_element_type=F32)
    for which, sem, count in ((r == 0, 0, 6), (r != 0, 0, 8), (wraps[1], 2, 2)):
        @pl.when(which)
        def _():
            whole(pool.at[pl.ds(ghosts, count * block_rows), :], send_sem.at[sem]).wait_send()

    whole(ghost, send_sem.at[1]).wait_send()


def local(positions, masses, occupancy, export_slots, export_count, pair_list, pair_count):
    leaves, width = masses.shape[1:]
    sent = export_slots.shape[1]
    pairs = pair_list.shape[2]
    return pl.pallas_call(
        kernel,
        out_shape=pltpu.VMEM(positions.shape, F32),
        in_specs=[pl.BlockSpec(memory_space=pl.ANY)] * 7,
        out_specs=pl.BlockSpec(memory_space=pltpu.VMEM),
        scratch_shapes=[
            pltpu.VMEM(positions.shape, F32),
            pltpu.VMEM(masses.shape, F32),
            pltpu.VMEM(occupancy.shape, jnp.int32),
            pltpu.SMEM(occupancy.shape, jnp.int32),
            pltpu.VMEM(export_slots.shape, jnp.int32),
            pltpu.SMEM(export_slots.shape, jnp.int32),
            pltpu.SMEM(export_count.shape, jnp.int32),
            pltpu.VMEM(pair_list.shape, jnp.int32),
            pltpu.SMEM(pair_list.shape, jnp.int32),
            pltpu.SMEM(pair_count.shape, jnp.int32),
            pltpu.VMEM((4 * (leaves + 8 * sent), width), F32),
            pltpu.VMEM((4 * sent, width), F32),
            pltpu.VMEM((leaves, width, 48), BF16),
            pltpu.VMEM((pairs, width, 2 * width), BF16),
            pltpu.VMEM((8 * leaves, width), F32),
            pltpu.VMEM((8 * pairs, width), F32),
            pltpu.VMEM((8 * pairs, width), F32),
            pltpu.VMEM((8, 3 * sent, width), F32),
            pltpu.VMEM((3, 8, sent, width), F32),
            pltpu.VMEM((2, 3 * sent, width), F32),
            pltpu.SemaphoreType.DMA((10,)),
            pltpu.SemaphoreType.DMA((3,)),
            pltpu.SemaphoreType.DMA((2 * CHUNKS + 2,)),
            pltpu.SemaphoreType.DMA((2, 3)),
        ],
        compiler_params=pltpu.CompilerParams(collective_id=0, has_side_effects=True),
    )(positions, masses, occupancy, export_slots, export_count, pair_list, pair_count)


def solution(mesh):
    return jax.shard_map(
        local,
        mesh=mesh,
        in_specs=(
            P(None, "space", "sub", None),
            P("space", "sub", None),
            P("space", "sub"),
            P("space", "sub"),
            P("space", "sub"),
            P(None, "space", "sub"),
            P("space", "sub"),
        ),
        out_specs=P(None, "space", "sub", None),
        check_vma=False,
    )
```

```python
import functools

import jax
import jax.numpy as jnp
from jax import lax
from jax.experimental import pallas as pl
from jax.experimental.pallas import tpu as pltpu
from jax.sharding import PartitionSpec as P

OFFSETS = ((-1, -1), (-1, 0), (-1, 1), (0, -1), (0, 1), (1, -1), (1, 0), (1, 1))
SOFTEN = 0.05
CENTRE = 0.75
MESH = pl.DeviceIdType.MESH
F32, BF16 = jnp.float32, jnp.bfloat16
UNROLL = 16
CHUNKS = 2
CUTS = (12, 16, 16)


def split3(v):
    high = v.astype(BF16).astype(F32)
    rest = v - high
    mid = rest.astype(BF16).astype(F32)
    return high, mid, rest - mid


def rows_of(sub, values):
    out = jnp.zeros(sub.shape, F32)
    for index, value in enumerate(values):
        out = jnp.where(sub == index, value, out)
    return out


def kernel(pos_in, mass_in, occ_in, slots_in, count_in, pairs_in, live_in, out,
           pos, mass, occ, occ_s, slots_v, slots_s, count_s, pairs_v, pairs_s, live_s,
           pool, export, turned, moments, kept, self_res, tgt_res, src_res, ghost, came, crossing, gathered,
           load_sem, send_sem, recv_sem, back_recv):
    leaves, width = mass.shape[1:]
    sent = slots_s.shape[1]
    pairs = pairs_s.shape[2]
    block_rows = 4 * sent
    own_blocks = leaves // sent
    n_space, n_sub = lax.axis_size("space"), lax.axis_size("sub")
    s, r = lax.axis_index("space"), lax.axis_index("sub")
    device = {
        (a, b): (lax.rem(s + n_space + a, n_space), lax.rem(r + n_sub + b, n_sub))
        for a, b in OFFSETS
    }
    wraps = {-1: r == 0, 1: r == n_sub - 1}
    edge = jnp.logical_or(wraps[-1], wraps[1])
    barrier = pltpu.get_barrier_semaphore()

    def greet(where):
        pl.semaphore_signal(barrier, inc=1, device_id=where, device_id_type=MESH)

    @pl.when(wraps[-1])
    def _():
        for a in (-1, 1):
            greet(device[(a, -1)])

    for where in ((0, -1), (0, 1), (-1, 0), (1, 0)):
        greet(device[where])
    loads = [
        pltpu.make_async_copy(source, target, load_sem.at[index])
        for index, (source, target) in enumerate((
            (slots_in, slots_s), (occ_in, occ_s), (count_in, count_s), (pos_in, pos),
            (mass_in, mass), (occ_in, occ), (slots_in, slots_v), (pairs_in, pairs_v),
            (pairs_in, pairs_s), (live_in, live_s),
        ))
    ]
    for copy in loads:
        copy.start()
    for copy in loads[:5]:
        copy.wait()

    def row(leaf, c):
        return lax.div(leaf, sent) * block_rows + lax.rem(leaf, sent) + c * sent

    def load(leaf):
        start = row(leaf, 0)
        return [pool[pl.ds(start + c * sent, 1), :] for c in range(4)]

    lane_row = lax.broadcasted_iota(jnp.int32, (1, width), 1)
    for g in range(sent):
        slot = slots_s[0, g]
        filled = jnp.where(g < count_s[0, 0], occ_s[0, slot], 0)
        for c in range(3):
            export[pl.ds(c * sent + g, 1), :] = pos[c, 0, pl.ds(slot, 1), :] - CENTRE
        export[pl.ds(3 * sent + g, 1), :] = jnp.where(
            lane_row < filled, mass[0, pl.ds(slot, 1), :], 0.0
        )

    sub = lax.broadcasted_iota(jnp.int32, (8, width), 0)
    low = sub < 4

    chunk_rows = block_rows // CHUNKS

    def rows_at(index, chunk=None):
        start = (own_blocks + OFFSETS.index(index)) * block_rows
        if chunk is None:
            return pl.ds(start, block_rows)
        return pl.ds(start + chunk * chunk_rows, chunk_rows)

    def send(source, where, target, sem, sent_sem=0):
        return pltpu.make_async_remote_copy(
            src_ref=source, dst_ref=pool.at[target, :], send_sem=send_sem.at[sent_sem],
            recv_sem=recv_sem.at[sem], device_id=device[where], device_id_type=MESH,
        )

    def whole(ref, sem):
        return pltpu.make_async_remote_copy(
            src_ref=ref, dst_ref=ref, send_sem=sem, recv_sem=sem,
            device_id=device[(0, 1)], device_id_type=MESH,
        )

    rest = 2 * CHUNKS
    across = {
        (a, chunk): send(
            export.at[pl.ds(chunk * chunk_rows, chunk_rows), :], (-a, 0),
            rows_at((a, 0), chunk), 2 * chunk + (a + 1) // 2,
        )
        for chunk in range(CHUNKS) for a in (-1, 1)
    }

    def forward(a, b, chunk):
        rows = rows_at((a, 0), chunk)
        return send(pool.at[rows, :], (0, -b), rows_at((a, b), chunk), rest)

    pl.semaphore_wait(barrier, jnp.where(wraps[1], 6, 4))
    @pl.when(wraps[1])
    def _():
        for a in (-1, 1):
            send(export, (-a, 1), rows_at((a, -1)), rest).start()

    for b in (1, -1):
        send(export, (0, -b), rows_at((0, b)), rest + (b + 1) // 2).start()
    for copy in across.values():
        copy.start()
    for copy in loads[5:]:
        copy.wait()
    eye = (
        lax.broadcasted_iota(jnp.int32, (leaves, leaves), 0)
        == lax.broadcasted_iota(jnp.int32, (leaves, leaves), 1)
    )
    occ_col = jnp.sum(jnp.where(eye, occ[...].astype(F32), 0.0), axis=1, keepdims=True)
    lane = lax.broadcasted_iota(jnp.int32, (leaves, width), 1).astype(F32)
    own_mass = jnp.where(lane < occ_col, mass[0], 0.0)
    for block in range(own_blocks):
        part = slice(block * sent, (block + 1) * sent)
        for c in range(3):
            pool[pl.ds(block * block_rows + c * sent, sent), :] = pos[c, 0, part] - CENTRE
        pool[pl.ds(block * block_rows + 3 * sent, sent), :] = own_mass[part]

    def load_twice(leaf):
        start = row(leaf, 0)
        four = pool[pl.ds(start, 4, stride=sent), :]
        return jnp.concatenate([four, four], axis=0), pool[pl.ds(start + 3 * sent, 1), :]

    def features(two):
        return jnp.where(low, jnp.where(sub == 3, 1.0, two), jnp.where(sub == 7, SOFTEN, two * two))

    def right_operand(vb):
        h, m, l = split3(vb)
        return jnp.concatenate([h, m, h, l, h, m], axis=0).astype(BF16)

    def left_operand(two, q):
        va = jnp.where(sub < 3, -2.0 * two, jnp.where(sub == 3, q, 1.0))
        h, m, l = split3(va)
        return jnp.concatenate([h, h, m, h, l, m], axis=0)

    ones = jnp.logical_or(sub == 3, sub == 7)

    def force_operand(two, m):
        moment = m * jnp.where(ones, 1.0, two)
        h, mid, l = split3(moment)
        both = jnp.concatenate([jnp.where(low, h, mid), jnp.where(low, l, 0.0)], axis=0).astype(BF16)
        return jnp.concatenate([both, both], axis=1)

    def weights(left, right):
        soft = jnp.dot(left, right, preferred_element_type=F32)
        fall = jnp.maximum((1.0 + SOFTEN) - soft, 0.0)
        root = lax.rsqrt(soft)
        part = fall * root
        return part * part * root

    def halves(weight):
        high = weight.astype(BF16)
        return high, (weight - high.astype(F32)).astype(BF16)

    def finish(product, vb, m):
        total = product[:8] + pltpu.roll(product[:8], 4, 0) + product[8:]
        return m * (total - vb * total[3:4])

    def self_pair(leaf):
        x, y, z, m = load(leaf)
        two, _ = load_twice(leaf)
        left = jnp.transpose(left_operand(two, x * x + y * y + z * z)).astype(BF16)
        turned[leaf] = left
        moment = force_operand(two, m)
        moments[leaf] = moment
        weight = weights(left, right_operand(features(two)))
        product = jnp.dot(
            moment, jnp.concatenate(halves(weight), axis=0), preferred_element_type=F32
        )
        self_res[pl.ds(pl.multiple_of(leaf * 8, 8), 8), :] = finish(product, two, m)

    def listed_pair(p):
        target, source = pairs_s[0, 0, p], pairs_s[1, 0, p]
        two, m = load_twice(source)
        weight = weights(turned[target], right_operand(features(two)))
        onto_source = jnp.dot(
            moments[target], jnp.concatenate(halves(weight), axis=0), preferred_element_type=F32
        )
        kept[p] = weight
        src_res[pl.ds(pl.multiple_of(p * 8, 8), 8), :] = finish(onto_source, two, m)

    def target_side(p):
        target, source = pairs_s[0, 0, p], pairs_s[1, 0, p]
        two_t, m_t = load_twice(target)
        two_u, m_u = load_twice(source)
        onto_target = lax.dot_general(
            force_operand(two_u, m_u), jnp.concatenate(halves(kept[p]), axis=1),
            (((1,), (1,)), ((), ())),
            preferred_element_type=F32,
        )
        tgt_res[pl.ds(pl.multiple_of(p * 8, 8), 8), :] = finish(onto_target, two_t, m_t)

    def run(body, first, last, unroll=UNROLL):
        def step(i, carry):
            for j in range(unroll):
                body(first + i * unroll + j)
            return carry

        lax.fori_loop(0, (last - first) // unroll, step, 0)

    cuts = [leaves * cut // 16 for cut in CUTS]
    run(self_pair, 0, cuts[0])
    for chunk in range(CHUNKS):
        for a in (-1, 1):
            across[(a, chunk)].wait_recv()
            for b in (-1, 1):
                @pl.when(jnp.logical_not(wraps[-b]))
                def _():
                    forward(a, b, chunk).start()
        run(self_pair, cuts[chunk], cuts[chunk + 1])
    ghosts = own_blocks * block_rows
    whole(pool.at[rows_at((0, 1)), :], recv_sem.at[rest + 1]).wait_recv()

    @pl.when(wraps[1])
    def _():
        for a in (-1, 1):
            send(pool.at[rows_at((0, 1)), :], (-a, 0), rows_at((a, 1)), rest, 2).start()

    whole(pool.at[pl.ds(ghosts, 5 * block_rows), :], recv_sem.at[rest]).wait_recv()
    run(listed_pair, 0, pairs, 64)

    def component(ref, c, count):
        return ref[pl.ds(c, count, stride=8), :]

    def stacked(values):
        return jnp.concatenate([part for part in split3(values)], axis=0).astype(BF16)

    pair_live = lax.broadcasted_iota(jnp.int32, (1, pairs), 1) < live_s[0, 0]

    def onehot(rows, start, wanted, live):
        which = lax.broadcasted_iota(jnp.int32, (rows, wanted.shape[1]), 0) + start
        hit = which == wanted
        if live is not None:
            hit = jnp.logical_and(hit, live)
        hit = jnp.where(hit, 1.0, 0.0)
        return hit

    tgt_row, src_row = pairs_v[0], pairs_v[1]
    src_parts = [stacked(component(src_res, c, pairs)) for c in range(3)]
    src_all = jnp.concatenate(src_parts, axis=1)
    hit = onehot(8 * sent, leaves, src_row, pair_live)
    onto_ghost = jnp.concatenate([hit, hit, hit], axis=1).astype(BF16)

    def part(c):
        return pl.ds(c * sent, sent)

    def slot_of(a, b):
        return {-1: 0, 1: 2, 0: 4}[a] + (b + 1) // 2

    def give(source, slot, where, c, last):
        return pltpu.make_async_remote_copy(
            src_ref=source, dst_ref=came.at[c, slot],
            send_sem=send_sem.at[1], recv_sem=back_recv.at[last, c],
            device_id=where, device_id_type=MESH,
        )

    def centre(b, c):
        source = ghost.at[OFFSETS.index((0, b)), part(c), :]
        return give(source, slot_of(0, b), device[(0, b)], c, 1)

    for c in range(3):
        ghost_force = jnp.dot(onto_ghost, src_parts[c], preferred_element_type=F32)
        for k in range(8):
            ghost[k, part(c), :] = ghost_force[k * sent:(k + 1) * sent]
        for a in (-1, 1):
            for b in (-1, 1):
                to_space, to_sub = device[(a, b)]
                slot, group = slot_of(a, b), jnp.where(wraps[b], 1, 0)
                if b < 0:
                    slot, group = jnp.where(wraps[b], 8 + (a + 1) // 2, slot), 2 * group
                    to_sub = jnp.where(wraps[b], r, to_sub)
                give(
                    ghost.at[OFFSETS.index((a, b)), part(c), :], slot,
                    (jnp.where(wraps[b], to_space, s), to_sub), c, group,
                ).start()

        @pl.when(wraps[1])
        def _():
            centre(1, c).start()

    for b in (-1, 1):
        @pl.when(jnp.logical_not(wraps[b]))
        def _():
            for c in range(3):
                centre(b, c).start()

    def took(c, last, which, there, elsewhere):
        for where, count in ((which, there), (jnp.logical_not(which), elsewhere)):
            @pl.when(where)
            def _():
                whole(came.at[c, pl.ds(0, count)], back_recv.at[last, c]).wait_recv()

    for c in range(3):
        took(c, 0, edge, 2, 4)

        for a in (-1, 1):
            side = (a + 1) // 2
            first = came[c, jnp.where(wraps[1], slot_of(a, 1), slot_of(a, -1))]
            second = came[c, jnp.where(wraps[-1], slot_of(a, -1), slot_of(a, 1))]
            crossing[side, part(c), :] = (
                ghost[OFFSETS.index((a, 0)), part(c), :] + first + jnp.where(edge, 0.0, second)
            )
            give(crossing.at[side, part(c), :], 6 + side, device[(a, 0)], c, 1).start()
    run(target_side, 0, pairs)

    @pl.when(wraps[-1])
    def _():
        for c in range(3):
            whole(came.at[c, pl.ds(8, 2)], back_recv.at[2, c]).wait_recv()
            gathered[part(c), :] = (
                ghost[OFFSETS.index((0, -1)), part(c), :] + came[c, 8] + came[c, 9]
            )
            give(gathered.at[part(c), :], slot_of(0, -1), device[(0, -1)], c, 1).start()

    tgt_all = jnp.concatenate([stacked(component(tgt_res, c, pairs)) for c in range(3)], axis=1)
    hit_t = onehot(leaves, 0, tgt_row, pair_live)
    hit_s = onehot(leaves, 0, src_row, pair_live)
    own_force = jnp.dot(
        jnp.concatenate([hit_t, hit_t, hit_t, hit_s, hit_s, hit_s], axis=1).astype(BF16),
        jnp.concatenate([tgt_all, src_all], axis=0), preferred_element_type=F32,
    )

    hit = onehot(leaves, 0, slots_v[...], None)
    onto_own = jnp.concatenate([hit, hit, hit], axis=1).astype(BF16)
    own_force = [
        component(self_res, c, leaves) + own_force[:, c * width:(c + 1) * width] for c in range(3)
    ]
    for c in range(3):
        took(c, 1, wraps[-1], 6, 4)

        far = [came[c, jnp.where(wraps[1], 4, slot_of(a, 1))] for a in (-1, 1)]
        returned = stacked(
            came[c, 4] + came[c, 5] + came[c, 6] + came[c, 7] + jnp.where(wraps[-1], far[0] + far[1], 0.0)
        )
        out[c, 0] = own_force[c] + jnp.dot(onto_own, returned, preferred_element_type=F32)
    for which, sem, count in ((r == 0, 0, 6), (r != 0, 0, 8), (wraps[1], 2, 2)):
        @pl.when(which)
        def _():
            whole(pool.at[pl.ds(ghosts, count * block_rows), :], send_sem.at[sem]).wait_send()

    whole(ghost, send_sem.at[1]).wait_send()


def local(positions, masses, occupancy, export_slots, export_count, pair_list, pair_count):
    leaves, width = masses.shape[1:]
    sent = export_slots.shape[1]
    pairs = pair_list.shape[2]
    return pl.pallas_call(
        kernel,
        out_shape=pltpu.VMEM(positions.shape, F32),
        in_specs=[pl.BlockSpec(memory_space=pl.ANY)] * 7,
        out_specs=pl.BlockSpec(memory_space=pltpu.VMEM),
        scratch_shapes=[
            pltpu.VMEM(positions.shape, F32),
            pltpu.VMEM(masses.shape, F32),
            pltpu.VMEM(occupancy.shape, jnp.int32),
            pltpu.SMEM(occupancy.shape, jnp.int32),
            pltpu.VMEM(export_slots.shape, jnp.int32),
            pltpu.SMEM(export_slots.shape, jnp.int32),
            pltpu.SMEM(export_count.shape, jnp.int32),
            pltpu.VMEM(pair_list.shape, jnp.int32),
            pltpu.SMEM(pair_list.shape, jnp.int32),
            pltpu.SMEM(pair_count.shape, jnp.int32),
            pltpu.VMEM((4 * (leaves + 8 * sent), width), F32),
            pltpu.VMEM((4 * sent, width), F32),
            pltpu.VMEM((leaves, width, 48), BF16),
            pltpu.VMEM((leaves, 16, 2 * width), BF16),
            pltpu.VMEM((pairs, width, width), F32),
            pltpu.VMEM((8 * leaves, width), F32),
            pltpu.VMEM((8 * pairs, width), F32),
            pltpu.VMEM((8 * pairs, width), F32),
            pltpu.VMEM((8, 3 * sent, width), F32),
            pltpu.VMEM((3, 10, sent, width), F32),
            pltpu.VMEM((2, 3 * sent, width), F32),
            pltpu.VMEM((3 * sent, width), F32),
            pltpu.SemaphoreType.DMA((10,)),
            pltpu.SemaphoreType.DMA((3,)),
            pltpu.SemaphoreType.DMA((2 * CHUNKS + 2,)),
            pltpu.SemaphoreType.DMA((3, 3)),
        ],
        compiler_params=pltpu.CompilerParams(collective_id=0, has_side_effects=True),
    )(positions, masses, occupancy, export_slots, export_count, pair_list, pair_count)


def solution(mesh):
    return jax.shard_map(
        local,
        mesh=mesh,
        in_specs=(
            P(None, "space", "sub", None),
            P("space", "sub", None),
            P("space", "sub"),
            P("space", "sub"),
            P("space", "sub"),
            P(None, "space", "sub"),
            P("space", "sub"),
        ),
        out_specs=P(None, "space", "sub", None),
        check_vma=False,
    )
```

```python
import functools

import jax
import jax.numpy as jnp
from jax import lax
from jax.experimental import pallas as pl
from jax.experimental.pallas import tpu as pltpu
from jax.sharding import PartitionSpec as P

OFFSETS = ((-1, -1), (-1, 0), (-1, 1), (0, -1), (0, 1), (1, -1), (1, 0), (1, 1))
SOFTEN = 0.05
CENTRE = 0.75
MESH = pl.DeviceIdType.MESH
F32, BF16 = jnp.float32, jnp.bfloat16
UNROLL = 16
CHUNKS = 2
CUTS = (12, 16, 16)


def split3(v):
    high = v.astype(BF16).astype(F32)
    rest = v - high
    mid = rest.astype(BF16).astype(F32)
    return high, mid, rest - mid


def rows_of(sub, values):
    out = jnp.zeros(sub.shape, F32)
    for index, value in enumerate(values):
        out = jnp.where(sub == index, value, out)
    return out


def kernel(pos_in, mass_in, occ_in, slots_in, count_in, pairs_in, live_in, out,
           pos, mass, occ, occ_s, slots_v, slots_s, count_s, pairs_v, pairs_s, live_s,
           pool, export, turned, moments, kept, self_res, tgt_res, src_res, ghost, came, crossing, gathered,
           load_sem, send_sem, recv_sem, back_recv):
    leaves, width = mass.shape[1:]
    sent = slots_s.shape[1]
    pairs = pairs_s.shape[2]
    block_rows = 4 * sent
    own_blocks = leaves // sent
    n_space, n_sub = lax.axis_size("space"), lax.axis_size("sub")
    s, r = lax.axis_index("space"), lax.axis_index("sub")
    device = {
        (a, b): (lax.rem(s + n_space + a, n_space), lax.rem(r + n_sub + b, n_sub))
        for a, b in OFFSETS
    }
    wraps = {-1: r == 0, 1: r == n_sub - 1}
    edge = jnp.logical_or(wraps[-1], wraps[1])
    barrier = pltpu.get_barrier_semaphore()

    def greet(where):
        pl.semaphore_signal(barrier, inc=1, device_id=where, device_id_type=MESH)

    @pl.when(wraps[-1])
    def _():
        for a in (-1, 1):
            greet(device[(a, -1)])

    for where in ((0, -1), (0, 1), (-1, 0), (1, 0)):
        greet(device[where])
    loads = [
        pltpu.make_async_copy(source, target, load_sem.at[index])
        for index, (source, target) in enumerate((
            (slots_in, slots_s), (occ_in, occ_s), (count_in, count_s), (pos_in, pos),
            (mass_in, mass), (occ_in, occ), (slots_in, slots_v), (pairs_in, pairs_v),
            (pairs_in, pairs_s), (live_in, live_s),
        ))
    ]
    for copy in loads:
        copy.start()
    for copy in loads[:5]:
        copy.wait()

    def row(leaf, c):
        return lax.div(leaf, sent) * block_rows + lax.rem(leaf, sent) + c * sent

    def load(leaf):
        start = row(leaf, 0)
        return [pool[pl.ds(start + c * sent, 1), :] for c in range(4)]

    lane_row = lax.broadcasted_iota(jnp.int32, (1, width), 1)
    for g in range(sent):
        slot = slots_s[0, g]
        filled = jnp.where(g < count_s[0, 0], occ_s[0, slot], 0)
        for c in range(3):
            export[pl.ds(c * sent + g, 1), :] = pos[c, 0, pl.ds(slot, 1), :] - CENTRE
        export[pl.ds(3 * sent + g, 1), :] = jnp.where(
            lane_row < filled, mass[0, pl.ds(slot, 1), :], 0.0
        )

    sub = lax.broadcasted_iota(jnp.int32, (8, width), 0)
    low = sub < 4

    chunk_rows = block_rows // CHUNKS

    def rows_at(index, chunk=None):
        start = (own_blocks + OFFSETS.index(index)) * block_rows
        if chunk is None:
            return pl.ds(start, block_rows)
        return pl.ds(start + chunk * chunk_rows, chunk_rows)

    def send(source, where, target, sem, sent_sem=0):
        return pltpu.make_async_remote_copy(
            src_ref=source, dst_ref=pool.at[target, :], send_sem=send_sem.at[sent_sem],
            recv_sem=recv_sem.at[sem], device_id=device[where], device_id_type=MESH,
        )

    def whole(ref, sem):
        return pltpu.make_async_remote_copy(
            src_ref=ref, dst_ref=ref, send_sem=sem, recv_sem=sem,
            device_id=device[(0, 1)], device_id_type=MESH,
        )

    rest = 2 * CHUNKS
    across = {
        (a, chunk): send(
            export.at[pl.ds(chunk * chunk_rows, chunk_rows), :], (-a, 0),
            rows_at((a, 0), chunk), 2 * chunk + (a + 1) // 2,
        )
        for chunk in range(CHUNKS) for a in (-1, 1)
    }

    def forward(a, b, chunk):
        rows = rows_at((a, 0), chunk)
        return send(pool.at[rows, :], (0, -b), rows_at((a, b), chunk), rest)

    pl.semaphore_wait(barrier, jnp.where(wraps[1], 6, 4))
    @pl.when(wraps[1])
    def _():
        for a in (-1, 1):
            send(export, (-a, 1), rows_at((a, -1)), rest).start()

    for b in (1, -1):
        send(export, (0, -b), rows_at((0, b)), rest + (b + 1) // 2).start()
    for copy in across.values():
        copy.start()
    for copy in loads[5:]:
        copy.wait()
    eye = (
        lax.broadcasted_iota(jnp.int32, (leaves, leaves), 0)
        == lax.broadcasted_iota(jnp.int32, (leaves, leaves), 1)
    )
    occ_col = jnp.sum(jnp.where(eye, occ[...].astype(F32), 0.0), axis=1, keepdims=True)
    lane = lax.broadcasted_iota(jnp.int32, (leaves, width), 1).astype(F32)
    own_mass = jnp.where(lane < occ_col, mass[0], 0.0)
    for block in range(own_blocks):
        part = slice(block * sent, (block + 1) * sent)
        for c in range(3):
            pool[pl.ds(block * block_rows + c * sent, sent), :] = pos[c, 0, part] - CENTRE
        pool[pl.ds(block * block_rows + 3 * sent, sent), :] = own_mass[part]

    def load_twice(leaf):
        start = row(leaf, 0)
        four = pool[pl.ds(start, 4, stride=sent), :]
        return jnp.concatenate([four, four], axis=0), pool[pl.ds(start + 3 * sent, 1), :]

    def features(two):
        return jnp.where(low, jnp.where(sub == 3, 1.0, two), jnp.where(sub == 7, SOFTEN, two * two))

    def right_operand(vb):
        h, m, l = split3(vb)
        return jnp.concatenate([h, m, h, l, h, m], axis=0).astype(BF16)

    def left_operand(two, q):
        va = jnp.where(sub < 3, -2.0 * two, jnp.where(sub == 3, q, 1.0))
        h, m, l = split3(va)
        return jnp.concatenate([h, h, m, h, l, m], axis=0)

    ones = jnp.logical_or(sub == 3, sub == 7)

    def force_operand(two, m):
        moment = m * jnp.where(ones, 1.0, two)
        h, mid, l = split3(moment)
        both = jnp.concatenate([jnp.where(low, h, mid), jnp.where(low, l, 0.0)], axis=0).astype(BF16)
        return jnp.concatenate([both, both], axis=1)

    def weights(left, right):
        soft = jnp.dot(left, right, preferred_element_type=F32)
        fall = jnp.maximum((1.0 + SOFTEN) - soft, 0.0)
        root = lax.rsqrt(soft)
        part = fall * root
        return part * part * root

    def halves(weight):
        high = weight.astype(BF16)
        return high, (weight - high.astype(F32)).astype(BF16)

    def finish(product, vb, m):
        total = product[:8] + pltpu.roll(product[:8], 4, 0) + product[8:]
        return m * (total - vb * total[3:4])

    def self_pair(leaf):
        x, y, z, m = load(leaf)
        two, _ = load_twice(leaf)
        left = jnp.transpose(left_operand(two, x * x + y * y + z * z)).astype(BF16)
        turned[leaf] = left
        moment = force_operand(two, m)
        moments[leaf] = moment
        weight = weights(left, right_operand(features(two)))
        product = jnp.dot(
            moment, jnp.concatenate(halves(weight), axis=0), preferred_element_type=F32
        )
        self_res[pl.ds(pl.multiple_of(leaf * 8, 8), 8), :] = finish(product, two, m)

    def listed_pair(p):
        target, source = pairs_s[0, 0, p], pairs_s[1, 0, p]
        two, m = load_twice(source)
        weight = weights(turned[target], right_operand(features(two)))
        onto_source = jnp.dot(
            moments[target], jnp.concatenate(halves(weight), axis=0), preferred_element_type=F32
        )
        kept[p] = weight
        src_res[pl.ds(pl.multiple_of(p * 8, 8), 8), :] = finish(onto_source, two, m)

    def target_side(p):
        target, source = pairs_s[0, 0, p], pairs_s[1, 0, p]
        two_t, m_t = load_twice(target)
        two_u, m_u = load_twice(source)
        onto_target = lax.dot_general(
            force_operand(two_u, m_u), jnp.concatenate(halves(kept[p]), axis=1),
            (((1,), (1,)), ((), ())),
            preferred_element_type=F32,
        )
        tgt_res[pl.ds(pl.multiple_of(p * 8, 8), 8), :] = finish(onto_target, two_t, m_t)

    def run(body, first, last, unroll=UNROLL):
        def step(i, carry):
            for j in range(unroll):
                body(first + i * unroll + j)
            return carry

        lax.fori_loop(0, (last - first) // unroll, step, 0)

    cuts = [leaves * cut // 16 for cut in CUTS]
    run(self_pair, 0, cuts[0])
    for chunk in range(CHUNKS):
        for a in (-1, 1):
            across[(a, chunk)].wait_recv()
            for b in (-1, 1):
                @pl.when(jnp.logical_not(wraps[-b]))
                def _():
                    forward(a, b, chunk).start()
        run(self_pair, cuts[chunk], cuts[chunk + 1])
    ghosts = own_blocks * block_rows
    whole(pool.at[rows_at((0, 1)), :], recv_sem.at[rest + 1]).wait_recv()

    @pl.when(wraps[1])
    def _():
        for a in (-1, 1):
            send(pool.at[rows_at((0, 1)), :], (-a, 0), rows_at((a, 1)), rest, 2).start()

    whole(pool.at[pl.ds(ghosts, 5 * block_rows), :], recv_sem.at[rest]).wait_recv()
    run(listed_pair, 0, pairs, 64)

    def component(ref, c, count):
        return ref[pl.ds(c, count, stride=8), :]

    def stacked(values):
        return jnp.concatenate([part for part in split3(values)], axis=0).astype(BF16)

    pair_live = lax.broadcasted_iota(jnp.int32, (1, pairs), 1) < live_s[0, 0]

    def onehot(rows, start, wanted, live):
        which = lax.broadcasted_iota(jnp.int32, (rows, wanted.shape[1]), 0) + start
        hit = which == wanted
        if live is not None:
            hit = jnp.logical_and(hit, live)
        hit = jnp.where(hit, 1.0, 0.0)
        return hit

    tgt_row, src_row = pairs_v[0], pairs_v[1]
    src_parts = [stacked(component(src_res, c, pairs)) for c in range(3)]
    src_all = jnp.concatenate(src_parts, axis=1)
    hit = onehot(8 * sent, leaves, src_row, pair_live)
    onto_ghost = jnp.concatenate([hit, hit, hit], axis=1).astype(BF16)

    def part(c):
        return pl.ds(c * sent, sent)

    def slot_of(a, b):
        return {-1: 0, 1: 2, 0: 4}[a] + (b + 1) // 2

    def give(source, slot, where, c, sem):
        return pltpu.make_async_remote_copy(
            src_ref=source, dst_ref=came.at[c, slot],
            send_sem=send_sem.at[1], recv_sem=back_recv.at[sem],
            device_id=where, device_id_type=MESH,
        )

    def centre(b, c):
        source = ghost.at[OFFSETS.index((0, b)), part(c), :]
        return give(source, slot_of(0, b), device[(0, b)], c, 3 + c)

    for c in range(3):
        ghost_force = jnp.dot(onto_ghost, src_parts[c], preferred_element_type=F32)
        for k in range(8):
            ghost[k, part(c), :] = ghost_force[k * sent:(k + 1) * sent]
        for a in (-1, 1):
            for b in (-1, 1):
                to_space, to_sub = device[(a, b)]
                slot, sem = slot_of(a, b), jnp.where(wraps[b], 3 + c, c)
                if b < 0:
                    slot, sem = jnp.where(wraps[b], 8 + (a + 1) // 2, slot), jnp.where(wraps[b], 6, c)
                    to_sub = jnp.where(wraps[b], r, to_sub)
                give(
                    ghost.at[OFFSETS.index((a, b)), part(c), :], slot,
                    (jnp.where(wraps[b], to_space, s), to_sub), c, sem,
                ).start()

        @pl.when(wraps[1])
        def _():
            centre(1, c).start()

    for b in (-1, 1):
        @pl.when(jnp.logical_not(wraps[b]))
        def _():
            for c in range(3):
                centre(b, c).start()

    def took(c, last, which, there, elsewhere):
        for where, count in ((which, there), (jnp.logical_not(which), elsewhere)):
            @pl.when(where)
            def _():
                whole(came.at[c, pl.ds(0, count)], back_recv.at[3 * last + c]).wait_recv()

    for c in range(3):
        took(c, 0, edge, 2, 4)

        for a in (-1, 1):
            side = (a + 1) // 2
            first = came[c, jnp.where(wraps[1], slot_of(a, 1), slot_of(a, -1))]
            second = came[c, jnp.where(wraps[-1], slot_of(a, -1), slot_of(a, 1))]
            crossing[side, part(c), :] = (
                ghost[OFFSETS.index((a, 0)), part(c), :] + first + jnp.where(edge, 0.0, second)
            )
            give(crossing.at[side, part(c), :], 6 + side, device[(a, 0)], c, 3 + c).start()
    run(target_side, 0, pairs)

    @pl.when(wraps[-1])
    def _():
        whole(came.at[0, pl.ds(0, 6)], back_recv.at[6]).wait_recv()
        for c in range(3):
            gathered[part(c), :] = (
                ghost[OFFSETS.index((0, -1)), part(c), :] + came[c, 8] + came[c, 9]
            )
            give(gathered.at[part(c), :], slot_of(0, -1), device[(0, -1)], c, 3 + c).start()

    tgt_all = jnp.concatenate([stacked(component(tgt_res, c, pairs)) for c in range(3)], axis=1)
    hit_t = onehot(leaves, 0, tgt_row, pair_live)
    hit_s = onehot(leaves, 0, src_row, pair_live)
    own_force = jnp.dot(
        jnp.concatenate([hit_t, hit_t, hit_t, hit_s, hit_s, hit_s], axis=1).astype(BF16),
        jnp.concatenate([tgt_all, src_all], axis=0), preferred_element_type=F32,
    )

    hit = onehot(leaves, 0, slots_v[...], None)
    onto_own = jnp.concatenate([hit, hit, hit], axis=1).astype(BF16)
    own_force = [
        component(self_res, c, leaves) + own_force[:, c * width:(c + 1) * width] for c in range(3)
    ]
    for c in range(3):
        took(c, 1, wraps[-1], 6, 4)

        far = [came[c, jnp.where(wraps[1], 4, slot_of(a, 1))] for a in (-1, 1)]
        returned = stacked(
            came[c, 4] + came[c, 5] + came[c, 6] + came[c, 7] + jnp.where(wraps[-1], far[0] + far[1], 0.0)
        )
        out[c, 0] = own_force[c] + jnp.dot(onto_own, returned, preferred_element_type=F32)
    for which, sem, count in ((r == 0, 0, 6), (r != 0, 0, 8), (wraps[1], 2, 2)):
        @pl.when(which)
        def _():
            whole(pool.at[pl.ds(ghosts, count * block_rows), :], send_sem.at[sem]).wait_send()

    whole(ghost, send_sem.at[1]).wait_send()


def local(positions, masses, occupancy, export_slots, export_count, pair_list, pair_count):
    leaves, width = masses.shape[1:]
    sent = export_slots.shape[1]
    pairs = pair_list.shape[2]
    return pl.pallas_call(
        kernel,
        out_shape=pltpu.VMEM(positions.shape, F32),
        in_specs=[pl.BlockSpec(memory_space=pl.ANY)] * 7,
        out_specs=pl.BlockSpec(memory_space=pltpu.VMEM),
        scratch_shapes=[
            pltpu.VMEM(positions.shape, F32),
            pltpu.VMEM(masses.shape, F32),
            pltpu.VMEM(occupancy.shape, jnp.int32),
            pltpu.SMEM(occupancy.shape, jnp.int32),
            pltpu.VMEM(export_slots.shape, jnp.int32),
            pltpu.SMEM(export_slots.shape, jnp.int32),
            pltpu.SMEM(export_count.shape, jnp.int32),
            pltpu.VMEM(pair_list.shape, jnp.int32),
            pltpu.SMEM(pair_list.shape, jnp.int32),
            pltpu.SMEM(pair_count.shape, jnp.int32),
            pltpu.VMEM((4 * (leaves + 8 * sent), width), F32),
            pltpu.VMEM((4 * sent, width), F32),
            pltpu.VMEM((leaves, width, 48), BF16),
            pltpu.VMEM((leaves, 16, 2 * width), BF16),
            pltpu.VMEM((pairs, width, width), F32),
            pltpu.VMEM((8 * leaves, width), F32),
            pltpu.VMEM((8 * pairs, width), F32),
            pltpu.VMEM((8 * pairs, width), F32),
            pltpu.VMEM((8, 3 * sent, width), F32),
            pltpu.VMEM((3, 10, sent, width), F32),
            pltpu.VMEM((2, 3 * sent, width), F32),
            pltpu.VMEM((3 * sent, width), F32),
            pltpu.SemaphoreType.DMA((10,)),
            pltpu.SemaphoreType.DMA((3,)),
            pltpu.SemaphoreType.DMA((2 * CHUNKS + 2,)),
            pltpu.SemaphoreType.DMA((7,)),
        ],
        compiler_params=pltpu.CompilerParams(
            collective_id=0, has_side_effects=True,
        ),
    )(positions, masses, occupancy, export_slots, export_count, pair_list, pair_count)


def solution(mesh):
    return jax.shard_map(
        local,
        mesh=mesh,
        in_specs=(
            P(None, "space", "sub", None),
            P("space", "sub", None),
            P("space", "sub"),
            P("space", "sub"),
            P("space", "sub"),
            P(None, "space", "sub"),
            P("space", "sub"),
        ),
        out_specs=P(None, "space", "sub", None),
        check_vma=False,
    )
```
